32 devices in a mesh: gx: 4 (over y, x), gy: 4 (over z), gz: 2 (over core).
Axes of the slice: x: 2, y: 2, z: 4, core: 2. Of those that a mesh axis runs over, the one named last changes fastest.
Arguments:
- load: float32 [256, 256, 256], P('gx', 'gy', 'gz'), may hold values from -12 to 12
- stiffness: float32 [256, 256, 256], P('gx', 'gy', 'gz'), may hold values from 0.02 to 2
- prestress: float32 [256, 256], P(('gx', 'gy'), 'gz'), may hold values from -3 to 3
- state_var: float32 [256, 256], P(('gx', 'gy'), 'gz'), may hold values from -1 to 1
- normal_a: float32 [256, 256], P(('gx', 'gy'), 'gz'), may hold values from 1 to 3
Outputs:
- displacement: float32 [256, 256, 256], P('gx', 'gy', 'gz')
- slip_rate: float32 [256, 256], P(('gx', 'gy'), 'gz')
The draws below stay inside these ranges and needn't reach their ends.
All inputs are finite; a program needn't handle non-finite values.
Results may differ from the reference program's by a relative error of at most 0.0003.
Values sent between devices are 32-bit elements; how exact they have to be, the bound alone decides.
A program may use at most 128 MiB of HBM per device.

```python
import math
import jax
import jax.numpy as jnp

ITERS = 3
NX = 256
NY = 256
NZ = 256


def draw_load(key, part):
    subkeys = jax.random.split(key, 4)
    along_x = ((jnp.arange(NX, dtype=jnp.float32) + 0.5) / NX)[:, None, None]
    along_y = ((jnp.arange(NY, dtype=jnp.float32) + 0.5) / NY)[None, :, None]
    along_z = ((jnp.arange(NZ, dtype=jnp.float32) + 0.5) / NZ)[None, None, :]
    waves_x = jax.random.randint(subkeys[0], (4,), 1, 4).astype(jnp.float32)
    waves_z = jax.random.randint(subkeys[1], (4,), 0, 2).astype(jnp.float32)
    phases = jax.random.uniform(subkeys[2], (7,), jnp.float32, 0.0, 2.0 * math.pi)
    smooth = jnp.zeros((NX, NY, NZ), jnp.float32)
    for mode_num in range(4):
        smooth = smooth + jnp.cos(2.0 * math.pi * (waves_x[mode_num] * along_x + along_y + waves_z[mode_num] * along_z) + phases[mode_num])
    smooth = smooth * 0.7071
    exponent = 0.5 + 0.25 * jnp.sin(2.0 * math.pi * along_x + phases[4]) + 0.25 * jnp.sin(2.0 * math.pi * along_y + phases[5])
    rough_scale = 0.3 * jnp.exp(exponent * math.log(5.0))
    smooth_scale = 0.4 + 0.4 * (1.0 + jnp.cos(2.0 * math.pi * along_z + phases[6]))
    white_noise = jax.random.truncated_normal(subkeys[3], -4.0, 4.0, (NX, NY, NZ), jnp.float32)
    return (smooth_scale * smooth + rough_scale * white_noise).astype(jnp.float32)


def level_of(rng, shape, cuts, smallest, top_value):
    factor_of = 1.0
    for dim, blocks in cuts:
        steps = jax.random.uniform(jax.random.fold_in(jax.random.fold_in(rng, 6), dim), (blocks,), jnp.float32, smallest / len(cuts), top_value / len(cuts))
        factor_of = factor_of * jnp.repeat(jnp.exp(steps), shape[dim] // blocks).reshape((-1,) + (1,) * (len(shape) - 1 - dim))
    return factor_of


def bell_draw(key, shape, spread, limit, cuts=(), kind=jnp.bfloat16):
    result = spread * jax.random.normal(key, shape, jnp.float32)
    if cuts:
        result = result * level_of(key, shape, cuts, -0.22, 0.18)
    return jnp.clip(result, -limit, limit).astype(kind)


def setup_inputs(seed: int = 0) -> dict:
    key_list = jax.random.split(jax.random.key(seed), 6)
    return {
        "load": draw_load(jax.random.fold_in(key_list[5], 71), 0),
        "stiffness": jnp.clip(jnp.exp(math.log(2.0) - 4.6051702 * jax.random.uniform(key_list[1], (NX, NY, NZ), jnp.float32) ** level_of(key_list[1], (NX, NY, NZ), ((0, 4), (1, 4), (2, 2)), -0.2, 0.2)), 0.02, 2.0),
        "prestress": bell_draw(key_list[2], (NX, NZ), 1.0, 3.0, ((0, 16), (1, 2)), jnp.float32),
        "state_var": jnp.clip(jax.random.uniform(key_list[3], (NX, NZ), jnp.float32, -1.0, 1.0) * level_of(key_list[3], (NX, NZ), ((0, 16), (1, 2)), -0.4, 0.0), -1.0, 1.0),
        "normal_a": jnp.clip(jnp.exp(math.log(3.0) - 1.0986123 * jax.random.uniform(key_list[4], (NX, NZ), jnp.float32) ** level_of(key_list[4], (NX, NZ), ((0, 16), (1, 2)), -0.2, 0.2)), 1.0, 3.0),
    }


def shifted(padded, sizes_now, axis_num, offset):
    slicers = [slice(2, 2 + sizes_now[0]), slice(2, 2 + sizes_now[1]), slice(2, 2 + sizes_now[2])]
    slicers[axis_num] = slice(2 + offset, 2 + offset + sizes_now[axis_num])
    return padded[tuple(slicers)]


def operate(field, stiffness):
    padded = jnp.pad(field, 2)
    sizes_now = field.shape
    near_sum = jnp.zeros_like(field)
    for axis_num in range(3):
        near_sum = near_sum + 16.0 * (shifted(padded, sizes_now, axis_num, 1) + shifted(padded, sizes_now, axis_num, -1))
        near_sum = near_sum - (shifted(padded, sizes_now, axis_num, 2) + shifted(padded, sizes_now, axis_num, -2))
    return (7.5 + stiffness) * field - near_sum / 12.0


def reference(load, stiffness, prestress, state_var, normal_a):
    inverse = 1.0 / (7.5 + stiffness)
    solution = jnp.zeros_like(load)
    residual = load
    precond = inverse * residual
    direction = precond
    gamma = jnp.sum(residual * precond)
    for iteration in range(ITERS):
        image = operate(direction, stiffness)
        alpha = gamma / jnp.sum(direction * image)
        solution = solution + alpha * direction
        residual = residual - alpha * image
        if iteration + 1 < ITERS:
            precond = inverse * residual
            gamma_new = jnp.sum(residual * precond)
            direction = precond + (gamma_new / gamma) * direction
            gamma = gamma_new
    half = NY // 2
    traction = (solution[:, half - 2, :] - 27.0 * solution[:, half - 1, :]
                + 27.0 * solution[:, half, :] - solution[:, half + 1, :]) / 24.0
    slip_rate = jnp.exp(-state_var) * jnp.sinh((prestress + 2.0 * traction) / normal_a)
    return solution, slip_rate
```

```python
import jax
import jax.numpy as jnp
from jax import lax
from jax.experimental import pallas as pl
from jax.experimental.pallas import tpu as pltpu
from jax.sharding import PartitionSpec as P

MESH = pl.DeviceIdType.MESH
AXES = ("gx", "gy", "gz")
PAD = 8
CHUNK = 8


def total(values):
    return jnp.sum(values.reshape(-1, 8, values.shape[-1]), axis=0)


def solve(t0, s):
    t1 = t0 - s[0]
    t2 = t1 - s[1]
    tiny = 1e-7
    p0 = s[0]
    l10 = s[1] / p0
    l20 = s[2] / p0
    p1 = s[2] - l10 * s[1]
    q = s[3] - l20 * s[1]
    ok1 = p1 > tiny * s[2]
    i1 = jnp.where(ok1, 1.0 / jnp.where(ok1, p1, 1.0), 0.0)
    l21 = q * i1
    p2 = s[4] - l20 * s[2] - l21 * q
    ok2 = ok1 & (p2 > tiny * s[4])
    i2 = jnp.where(ok2, 1.0 / jnp.where(ok2, p2, 1.0), 0.0)
    y1 = t1 - l10 * t0
    y2 = t2 - l20 * t0 - l21 * y1
    c2 = y2 * i2
    c1 = y1 * i1 - l21 * c2
    c0 = t0 / p0 - l10 * c1 - l20 * c2
    return c0, c1, c2


def make_kernel(sizes):
    ngx, ngy, ngz = sizes
    count = ngx * ngy * ngz

    def kernel(load, stiff, pre_ref, state_ref, norm_ref, out, slip,
               b, d, u0, u1, u2, obuf, ysend, yrecv, zsend, zrecv, fsend, frecv, red,
               in_sem, out_sem, send_sem, recv_sem, fs_sem, fr_sem, rs_sem, rr_sem):
        nx, ny, nz = b.shape
        us = (u0, u1, u2)
        ix, iy, iz = (lax.axis_index(a) for a in AXES)
        me = (ix * ngy + iy) * ngz + iz
        spots = (ix, iy, iz)

        def other(step):
            who = lax.rem(me + step, count)
            return (who // (ngy * ngz), lax.rem(who // ngz, ngy), lax.rem(who, ngz))

        chunks = nx // CHUNK
        order = [0, chunks - 1] + list(range(1, chunks - 1))
        copies = {}
        for c in order:
            part = pl.ds(c * CHUNK, CHUNK)
            copies[c] = (
                pltpu.make_async_copy(load.at[part], b.at[part], in_sem.at[0, c]),
                pltpu.make_async_copy(stiff.at[part], d.at[part], in_sem.at[1, c]),
            )
            for one in copies[c]:
                one.start()

        barrier = pltpu.get_barrier_semaphore()

        @pl.loop(1, count)
        def _(step):
            pl.semaphore_signal(barrier, inc=1, device_id=other(step), device_id_type=MESH)

        zero_plane = jnp.zeros((2, ny, nz), jnp.float32)
        zero_rows = jnp.zeros((nx, 2, nz), jnp.float32)
        for k in range(3):
            @pl.when(ix == 0)
            def _():
                us[k][0:2, PAD:PAD + ny, :] = zero_plane
            @pl.when(ix == ngx - 1)
            def _():
                us[k][nx + 2:nx + 4, PAD:PAD + ny, :] = zero_plane
            @pl.when(iy == 0)
            def _():
                yrecv[k, 0] = zero_rows
            @pl.when(iy == ngy - 1)
            def _():
                yrecv[k, 1] = zero_rows

        lane = lax.broadcasted_iota(jnp.int32, (ny, nz), 1)
        first = iz == 0
        send_base = jnp.where(first, 2, 0)
        recv_base = jnp.where(first, nz, 2 * nz - 2)

        def place(field, x, value, k, pack):
            us[k][x + 2, PAD:PAD + ny, :] = value
            ysend[k, 0, x] = value[0:2]
            ysend[k, 1, x] = value[ny - 2:ny]
            moved = pltpu.roll(value, lax.rem(2 * x + send_base, nz), 1)
            return jnp.where((lane >> 1) == x, moved, pack)

        def xcopy(k, side):
            u = us[k]
            if side == 0:
                src, dst, to = u.at[2:4, PAD:PAD + ny], u.at[nx + 2:nx + 4, PAD:PAD + ny], ix - 1
            else:
                src, dst, to = u.at[nx:nx + 2, PAD:PAD + ny], u.at[0:2, PAD:PAD + ny], ix + 1
            return pltpu.make_async_remote_copy(
                src, dst, send_sem.at[k, side], recv_sem.at[k, side],
                device_id=(to, iy, iz), device_id_type=MESH)

        def ycopy(k, side):
            to = iy - 1 if side == 0 else iy + 1
            return pltpu.make_async_remote_copy(
                ysend.at[k, side], yrecv.at[k, 1 - side], send_sem.at[k, 2 + side],
                recv_sem.at[k, 2 + side], device_id=(ix, to, iz), device_id_type=MESH)

        def zcopy(k):
            return pltpu.make_async_remote_copy(
                zsend.at[k], zrecv.at[k], send_sem.at[k, 4], recv_sem.at[k, 4],
                device_id=(ix, iy, 1 - iz), device_id_type=MESH)

        def sending(spot, size, side):
            return spot > 0 if side == 0 else spot < size - 1

        def receiving(spot, size, side):
            return spot < size - 1 if side == 0 else spot > 0

        def sides(k):
            return (1,) if k == 2 else (0, 1)

        def each(make, k, spot, size, test, act):
            for side in sides(k):
                @pl.when(test(spot, size, side))
                def _():
                    act(make(k, side))

        def start_x(k):
            each(xcopy, k, ix, ngx, sending, lambda c: c.start())

        def start_yz(k):
            each(ycopy, k, iy, ngy, sending, lambda c: c.start())
            zcopy(k).start()

        def scale(x, carry):
            t0, pack = carry
            inv = 1.0 / (7.5 + d[x])
            d[x] = inv
            rhs = b[x]
            value = inv * rhs
            return t0 + total(value * rhs), place(u0, x, value, 0, pack)

        carry = (jnp.zeros((8, nz), jnp.float32), jnp.zeros((ny, nz), jnp.float32))
        for n, c in enumerate(order):
            for one in copies[c]:
                one.wait()
            carry = lax.fori_loop(c * CHUNK, (c + 1) * CHUNK, scale, carry)
            if n == 1:
                pl.semaphore_wait(barrier, count - 1)
                start_x(0)
        t0, pack = carry
        zsend[0] = pack
        start_yz(0)

        def wait_y(k):
            each(ycopy, k, iy, ngy, receiving, lambda c: c.wait_recv())

        def wait_x(k):
            each(xcopy, k, ix, ngx, receiving, lambda c: c.wait_recv())

        def ends(k, x, value):
            got = pltpu.roll(zrecv[k], lax.rem(recv_base - 2 * x, nz), 1)
            nothing = jnp.zeros_like(got)
            low = jnp.where(first, nothing, got)
            high = jnp.where(first, got, nothing)
            return (
                pltpu.roll(jnp.where(lane >= nz - 1, low, value), 1, 1),
                pltpu.roll(jnp.where(lane >= nz - 2, low, value), 2, 1),
                pltpu.roll(jnp.where(lane < 1, high, value), nz - 1, 1),
                pltpu.roll(jnp.where(lane < 2, high, value), nz - 2, 1),
            )

        def near(k, x):
            u = us[k]
            u[x + 2, PAD - 2:PAD, :] = yrecv[k, 0, x]
            u[x + 2, PAD + ny:PAD + ny + 2, :] = yrecv[k, 1, x]
            value = u[x + 2, PAD:PAD + ny, :]
            low1, low2, high1, high2 = ends(k, x, value)
            one = (u[x + 1, PAD:PAD + ny, :] + u[x + 3, PAD:PAD + ny, :]
                   + u[x + 2, PAD - 1:PAD - 1 + ny, :] + u[x + 2, PAD + 1:PAD + 1 + ny, :]
                   + low1 + high1)
            two = (u[x, PAD:PAD + ny, :] + u[x + 4, PAD:PAD + ny, :]
                   + u[x + 2, PAD - 2:PAD - 2 + ny, :] + u[x + 2, PAD + 2:PAD + 2 + ny, :]
                   + low2 + high2)
            return value, (16.0 * one - two) * (1.0 / 12.0)

        def half_near(k, x):
            u = us[k]
            u[x + 2, PAD - 2:PAD, :] = yrecv[k, 0, x]
            value = u[x + 2, PAD:PAD + ny, :]
            low1, low2, _, _ = ends(k, x, value)
            one = (u[x + 1, PAD:PAD + ny, :] + u[x + 2, PAD - 1:PAD - 1 + ny, :]
                   + low1)
            two = (u[x, PAD:PAD + ny, :] + u[x + 2, PAD - 2:PAD - 2 + ny, :]
                   + low2)
            return value, (16.0 * one - two) * (1.0 / 6.0)

        zero = jnp.zeros((8, nz), jnp.float32)

        def run(step, k, carry, low_edge, high_edge):
            carry = lax.fori_loop(2, nx - 2 if high_edge else nx, step, carry)
            wait_x(k)
            carry = lax.fori_loop(0, 2, step, carry)
            if high_edge:
                carry = lax.fori_loop(nx - 2, nx, step, carry)
            return carry

        def advance(k):
            def step(x, carry):
                even, odd, pack = carry
                value, w = near(k, x)
                fresh = d[x] * w
                even = even + total(value * (b[x] - w))
                odd = odd + total((value - fresh) * w)
                b[x] = w
                return even, odd, place(None, x, fresh, k + 1, pack)

            zcopy(k).wait_recv()
            wait_y(k)
            even, odd, pack = run(step, k, (zero, zero, jnp.zeros((ny, nz), jnp.float32)), True, True)
            start_x(k + 1)
            zsend[k + 1] = pack
            start_yz(k + 1)
            return even, odd

        s0, s1 = advance(0)
        s2, s3 = advance(1)

        owned = nx // ngy
        below = iy == ngy // 2 - 1
        above = iy == ngy // 2

        def fault_copy(which, to):
            return pltpu.make_async_remote_copy(
                fsend.at[:, pl.ds(to * owned, owned), :], frecv.at[which], fs_sem.at[to], fr_sem.at[which],
                device_id=(ix, to, iz), device_id_type=MESH)

        @pl.when(below | above)
        def _():
            edge = jnp.where(below, 1, 0)
            far = jnp.where(below, 1.0 / 24.0, 27.0 / 24.0)
            close = jnp.where(below, -27.0 / 24.0, -1.0 / 24.0)

            @pl.loop(0, nx)
            def _(x):
                for j in range(3):
                    rows = ysend[j, edge, x]
                    fsend[j, pl.ds(x, 1), :] = far * rows[0:1] + close * rows[1:2]

        for which, owner in enumerate((ngy // 2 - 1, ngy // 2)):
            @pl.when(iy == owner)
            def _():
                for to in range(ngy):
                    if to != owner:
                        fault_copy(which, to).start()
                frecv[which] = fsend[:, owner * owned:(owner + 1) * owned, :]

        def last(x, s4):
            value, w = half_near(2, x)
            return s4 + total(value * (b[x] - w))

        zcopy(2).wait_recv()
        wait_y(2)
        s4 = run(last, 2, zero, True, False)

        slot = lax.broadcasted_iota(jnp.int32, (1, nz), 1)
        row = jnp.zeros((1, nz), jnp.float32)
        for j, part in enumerate((t0, s0, s1, s2, s3, s4)):
            whole = jnp.sum(jnp.sum(part, axis=1, keepdims=True), axis=0, keepdims=True)
            row = row + jnp.where(slot == j, whole, 0.0)
        red[me] = row

        def sum_copy(step):
            return pltpu.make_async_remote_copy(
                red.at[me], red.at[me], rs_sem.at[step], rr_sem.at[me],
                device_id=other(step), device_id_type=MESH)

        @pl.loop(1, count)
        def _(step):
            sum_copy(step).start()

        @pl.loop(1, count)
        def _(step):
            who = lax.rem(me + step, count)
            pltpu.make_async_remote_copy(
                red.at[who], red.at[who], rs_sem.at[step], rr_sem.at[who],
                device_id=other(step), device_id_type=MESH).wait_recv()

        sums = jnp.sum(red[...], axis=0)
        parts = [jnp.sum(jnp.where(slot == j, sums, 0.0), axis=1, keepdims=True) for j in range(6)]
        coefs = [jnp.broadcast_to(c, (1, nz)) for c in solve(parts[0], parts[1:])]

        def out_copy(c):
            part = pl.ds(c * CHUNK, CHUNK)
            return pltpu.make_async_copy(obuf.at[part], out.at[part], out_sem.at[c])

        def blend(x, carry):
            mid = slice(PAD, PAD + ny)
            obuf[x] = (coefs[0] * u0[x + 2, mid, :] + coefs[1] * u1[x + 2, mid, :]
                       + coefs[2] * u2[x + 2, mid, :])
            return carry

        for c in range(chunks):
            lax.fori_loop(c * CHUNK, (c + 1) * CHUNK, blend, 0)
            out_copy(c).start()

        for which, owner in enumerate((ngy // 2 - 1, ngy // 2)):
            @pl.when(iy != owner)
            def _():
                fault_copy(which, owner).wait_recv()
        traction = sum(coefs[j] * (frecv[0, j] + frecv[1, j]) for j in range(3))
        arg = (pre_ref[...] + 2.0 * traction) / norm_ref[...]
        half = jnp.float32(-0.6931471805599453)
        small = arg * (1.0 + arg * arg * (1.0 / 6.0) * (1.0 + arg * arg * 0.05))
        sinh = jnp.where(jnp.abs(arg) < 0.25, small, jnp.exp(arg + half) - jnp.exp(half - arg))
        slip[...] = jnp.exp(-state_ref[...]) * sinh

        for k in range(3):
            each(xcopy, k, ix, ngx, sending, lambda c: c.wait_send())
            each(ycopy, k, iy, ngy, sending, lambda c: c.wait_send())
            zcopy(k).wait_send()
        for which, owner in enumerate((ngy // 2 - 1, ngy // 2)):
            @pl.when(iy == owner)
            def _():
                for to in range(ngy):
                    if to != owner:
                        fault_copy(which, to).wait_send()

        @pl.loop(1, count)
        def _(step):
            sum_copy(step).wait_send()

        for c in range(chunks):
            out_copy(c).wait()

    return kernel


def solution(mesh):
    sizes = tuple(mesh.shape[a] for a in AXES)
    assert sizes[1] % 2 == 0 and sizes[2] == 2

    def per_device(load, stiffness, prestress, state_var, normal_a):
        nx, ny, nz = load.shape
        assert 2 * nx <= nz and nx % CHUNK == 0
        f32 = jnp.float32
        count = sizes[0] * sizes[1] * sizes[2]
        padded = (nx + 4, ny + 2 * PAD, nz)
        vmem = pl.BlockSpec(memory_space=pltpu.VMEM)
        hbm = pl.BlockSpec(memory_space=pl.ANY)
        dma = pltpu.SemaphoreType.DMA
        return pl.pallas_call(
            make_kernel(sizes),
            out_shape=(
                jax.ShapeDtypeStruct(load.shape, f32),
                jax.ShapeDtypeStruct(prestress.shape, f32),
            ),
            in_specs=[hbm, hbm, vmem, vmem, vmem],
            out_specs=(hbm, vmem),
            scratch_shapes=[
                pltpu.VMEM((nx, ny, nz), f32),
                pltpu.VMEM((nx, ny, nz), f32),
                pltpu.VMEM(padded, f32),
                pltpu.VMEM(padded, f32),
                pltpu.VMEM(padded, f32),
                pltpu.VMEM((nx, ny, nz), f32),
                pltpu.VMEM((3, 2, nx, 2, nz), f32),
                pltpu.VMEM((3, 2, nx, 2, nz), f32),
                pltpu.VMEM((3, ny, nz), f32),
                pltpu.VMEM((3, ny, nz), f32),
                pltpu.VMEM((3, nx, nz), f32),
                pltpu.VMEM((2, 3, nx // sizes[1], nz), f32),
                pltpu.VMEM((count, 1, nz), f32),
                dma((2, nx // CHUNK)),
                dma((nx // CHUNK,)),
                dma((3, 5)),
                dma((3, 5)),
                dma((sizes[1],)),
                dma((2,)),
                dma((count,)),
                dma((count,)),
            ],
            compiler_params=pltpu.CompilerParams(collective_id=0, has_side_effects=True),
        )(load, stiffness, prestress, state_var, normal_a)

    placed = (
        P("gx", "gy", "gz"),
        P("gx", "gy", "gz"),
        P(("gx", "gy"), "gz"),
        P(("gx", "gy"), "gz"),
        P(("gx", "gy"), "gz"),
    )
    return jax.shard_map(
        per_device,
        mesh=mesh,
        in_specs=placed,
        out_specs=(P("gx", "gy", "gz"), P(("gx", "gy"), "gz")),
        check_vma=False,
    )
```

```python
import jax
import jax.numpy as jnp
from jax import lax
from jax.experimental import pallas as pl
from jax.experimental.pallas import tpu as pltpu
from jax.sharding import PartitionSpec as P

MESH = pl.DeviceIdType.MESH
AXES = ("gx", "gy", "gz")
PAD = 8
CHUNK = 8
GROUP = 2


def total(values):
    return jnp.sum(values.reshape(-1, 8, values.shape[-1]), axis=0)


def solve(t0, s):
    t1 = t0 - s[0]
    t2 = t1 - s[1]
    tiny = 1e-7
    p0 = s[0]
    l10 = s[1] / p0
    l20 = s[2] / p0
    p1 = s[2] - l10 * s[1]
    q = s[3] - l20 * s[1]
    ok1 = p1 > tiny * s[2]
    i1 = jnp.where(ok1, 1.0 / jnp.where(ok1, p1, 1.0), 0.0)
    l21 = q * i1
    p2 = s[4] - l20 * s[2] - l21 * q
    ok2 = ok1 & (p2 > tiny * s[4])
    i2 = jnp.where(ok2, 1.0 / jnp.where(ok2, p2, 1.0), 0.0)
    y1 = t1 - l10 * t0
    y2 = t2 - l20 * t0 - l21 * y1
    c2 = y2 * i2
    c1 = y1 * i1 - l21 * c2
    c0 = t0 / p0 - l10 * c1 - l20 * c2
    return c0, c1, c2


def parts_of(nx):
    inner = nx - 4
    runs = max(n for n in range(1, 7) if inner % (GROUP * n) == 0)
    size = inner // runs
    return [(0, 2), (nx - 2, 2)] + [(2 + n * size, size) for n in range(runs)]


def halves(values):
    high = values.astype(jnp.bfloat16)
    return high, (values - high.astype(jnp.float32)).astype(jnp.bfloat16)


def make_kernel(sizes):
    ngx, ngy, ngz = sizes
    count = ngx * ngy * ngz

    def kernel(load, stiff, pre_ref, state_ref, norm_ref, out, slip,
               b, d, u0, u1, u2, obuf, ysend, yrecv, zrecv, band, fsend, frecv, red,
               in_sem, out_sem, send_sem, recv_sem, zs_sem, zr_sem, fs_sem, fr_sem, rs_sem, rr_sem):
        nx, ny, nz = b.shape
        us = (u0, u1, u2)
        ix, iy, iz = (lax.axis_index(a) for a in AXES)
        me = (ix * ngy + iy) * ngz + iz
        spots = (ix, iy, iz)

        def other(step):
            who = lax.rem(me + step, count)
            return (who // (ngy * ngz), lax.rem(who // ngz, ngy), lax.rem(who, ngz))

        parts = parts_of(nx)
        copies = []
        for n, (at, size) in enumerate(parts):
            part = pl.ds(at, size)
            copies.append((
                pltpu.make_async_copy(load.at[part], b.at[part], in_sem.at[0, n]),
                pltpu.make_async_copy(stiff.at[part], d.at[part], in_sem.at[1, n]),
            ))
            for one in copies[n]:
                one.start()

        barrier = pltpu.get_barrier_semaphore()

        @pl.loop(1, count)
        def _(step):
            pl.semaphore_signal(barrier, inc=1, device_id=other(step), device_id_type=MESH)

        zero_plane = jnp.zeros((2, ny, nz), jnp.float32)
        zero_rows = jnp.zeros((nx, 2, nz), jnp.float32)
        for k in range(3):
            @pl.when(ix == 0)
            def _():
                us[k][0:2, PAD:PAD + ny, :] = zero_plane
            @pl.when(ix == ngx - 1)
            def _():
                us[k][nx + 2:nx + 4, PAD:PAD + ny, :] = zero_plane
            @pl.when(iy == 0)
            def _():
                yrecv[k, 0] = zero_rows
            @pl.when(iy == ngy - 1)
            def _():
                yrecv[k, 1] = zero_rows

        row = lax.broadcasted_iota(jnp.int32, (nz, nz), 0)
        col = lax.broadcasted_iota(jnp.int32, (nz, nz), 1)
        far = row + jnp.where(iz == 0, nz, -nz)
        for n, at in enumerate((row, far, row, far)):
            gap = col - at
            full = jnp.where(jnp.abs(gap) == 1, 16.0, 0.0) - jnp.where(jnp.abs(gap) == 2, 1.0, 0.0)
            half = jnp.where(gap == 1, 16.0, 0.0) - jnp.where(gap == 2, 1.0, 0.0)
            band[0, n * nz:(n + 1) * nz, :] = full.astype(jnp.bfloat16)
            band[1, n * nz:(n + 1) * nz, :] = half.astype(jnp.bfloat16)

        def place(x, value, k):
            us[k][x + 2, PAD:PAD + ny, :] = value
            ysend[k, 0, x] = value[0:2]
            ysend[k, 1, x] = value[ny - 2:ny]

        def xcopy(k, side):
            u = us[k]
            if side == 0:
                src, dst, to = u.at[2:4, PAD:PAD + ny], u.at[nx + 2:nx + 4, PAD:PAD + ny], ix - 1
            else:
                src, dst, to = u.at[nx:nx + 2, PAD:PAD + ny], u.at[0:2, PAD:PAD + ny], ix + 1
            return pltpu.make_async_remote_copy(
                src, dst, send_sem.at[k, side], recv_sem.at[k, side],
                device_id=(to, iy, iz), device_id_type=MESH)

        def ycopy(k, side):
            to = iy - 1 if side == 0 else iy + 1
            return pltpu.make_async_remote_copy(
                ysend.at[k, side], yrecv.at[k, 1 - side], send_sem.at[k, 2 + side],
                recv_sem.at[k, 2 + side], device_id=(ix, to, iz), device_id_type=MESH)

        def zcopy(k, at, size, n):
            return pltpu.make_async_remote_copy(
                us[k].at[pl.ds(at + 2, size), PAD:PAD + ny], zrecv.at[k, pl.ds(at, size)],
                zs_sem.at[k, n], zr_sem.at[k, n],
                device_id=(ix, iy, 1 - iz), device_id_type=MESH)

        def sending(spot, size, side):
            return spot > 0 if side == 0 else spot < size - 1

        def receiving(spot, size, side):
            return spot < size - 1 if side == 0 else spot > 0

        def sides(k):
            return (1,) if k == 2 else (0, 1)

        def each(make, k, spot, size, test, act):
            for side in sides(k):
                @pl.when(test(spot, size, side))
                def _():
                    act(make(k, side))

        def start_x(k):
            each(xcopy, k, ix, ngx, sending, lambda c: c.start())

        def start_y(k):
            each(ycopy, k, iy, ngy, sending, lambda c: c.start())

        def scale(x, t0):
            inv = 1.0 / (7.5 + d[x])
            d[x] = inv
            rhs = b[x]
            value = inv * rhs
            place(x, value, 0)
            return t0 + total(value * rhs)

        t0 = jnp.zeros((8, nz), jnp.float32)
        for n, (at, size) in enumerate(parts):
            for one in copies[n]:
                one.wait()
            t0 = lax.fori_loop(at, at + size, scale, t0)
            if n == 1:
                pl.semaphore_wait(barrier, count - 1)
                start_x(0)
                zcopy(0, *parts[0], 0).start()
            if n >= 1:
                zcopy(0, at, size, n).start()
        start_y(0)

        def wait_y(k):
            each(ycopy, k, iy, ngy, receiving, lambda c: c.wait_recv())

        def wait_x(k):
            each(xcopy, k, ix, ngx, receiving, lambda c: c.wait_recv())

        def along_z(k, x, which):
            own = us[k][pl.ds(x + 2, GROUP), PAD:PAD + ny, :].reshape(GROUP * ny, nz)
            next_to = zrecv[k, pl.ds(x, GROUP)].reshape(GROUP * ny, nz)
            own_high, own_low = halves(own)
            next_high, next_low = halves(next_to)
            lhs = jnp.concatenate([own_high, next_high, own_low, next_low], axis=1)
            return jnp.dot(lhs, band[which], preferred_element_type=jnp.float32)

        def near(k, x, z_term):
            u = us[k]
            u[x + 2, PAD - 2:PAD, :] = yrecv[k, 0, x]
            u[x + 2, PAD + ny:PAD + ny + 2, :] = yrecv[k, 1, x]
            one = (u[x + 1, PAD:PAD + ny, :] + u[x + 3, PAD:PAD + ny, :]
                   + u[x + 2, PAD - 1:PAD - 1 + ny, :] + u[x + 2, PAD + 1:PAD + 1 + ny, :])
            two = (u[x, PAD:PAD + ny, :] + u[x + 4, PAD:PAD + ny, :]
                   + u[x + 2, PAD - 2:PAD - 2 + ny, :] + u[x + 2, PAD + 2:PAD + 2 + ny, :])
            return (16.0 * one - two + z_term) * (1.0 / 12.0)

        def half_near(k, x, z_term):
            u = us[k]
            u[x + 2, PAD - 2:PAD, :] = yrecv[k, 0, x]
            one = u[x + 1, PAD:PAD + ny, :] + u[x + 2, PAD - 1:PAD - 1 + ny, :]
            two = u[x, PAD:PAD + ny, :] + u[x + 2, PAD - 2:PAD - 2 + ny, :]
            return (16.0 * one - two + z_term) * (1.0 / 6.0)

        zero = jnp.zeros((8, nz), jnp.float32)

        def run(plane, k, carry, which, done):
            def group(at, n, carry):
                x = at + n * GROUP
                z_terms = along_z(k, x, which)
                for g in range(GROUP):
                    carry = plane(x + g, z_terms[g * ny:(g + 1) * ny], carry)
                return carry

            def part(at, size, n, carry):
                zcopy(k, at, size, n).wait_recv()
                carry = lax.fori_loop(0, size // GROUP, lambda i, c: group(at, i, c), carry)
                done(at, size, n)
                return carry

            first_at, size = parts[2]
            carry = lax.fori_loop(
                0, len(parts) - 2, lambda n, c: part(first_at + n * size, size, n + 2, c), carry)
            wait_x(k)
            for n in range(2):
                carry = part(*parts[n], n, carry)
            return carry

        def advance(k):
            def plane(x, z_term, carry):
                even, odd = carry
                value = us[k][x + 2, PAD:PAD + ny, :]
                w = near(k, x, z_term)
                fresh = d[x] * w
                even = even + total(value * (b[x] - w))
                odd = odd + total((value - fresh) * w)
                b[x] = w
                place(x, fresh, k + 1)
                return even, odd

            wait_y(k)
            even, odd = run(plane, k, (zero, zero), 0, lambda *p: zcopy(k + 1, *p).start())
            start_x(k + 1)
            start_y(k + 1)
            return even, odd

        s0, s1 = advance(0)
        s2, s3 = advance(1)

        owned = nx // ngy
        below = iy == ngy // 2 - 1
        above = iy == ngy // 2

        def fault_copy(which, to):
            return pltpu.make_async_remote_copy(
                fsend.at[:, pl.ds(to * owned, owned), :], frecv.at[which], fs_sem.at[to], fr_sem.at[which],
                device_id=(ix, to, iz), device_id_type=MESH)

        @pl.when(below | above)
        def _():
            edge = jnp.where(below, 1, 0)
            front = jnp.where(below, 1.0 / 24.0, 27.0 / 24.0)
            close = jnp.where(below, -27.0 / 24.0, -1.0 / 24.0)

            @pl.loop(0, nx)
            def _(x):
                for j in range(3):
                    rows = ysend[j, edge, x]
                    fsend[j, pl.ds(x, 1), :] = front * rows[0:1] + close * rows[1:2]

        for which, owner in enumerate((ngy // 2 - 1, ngy // 2)):
            @pl.when(iy == owner)
            def _():
                for to in range(ngy):
                    if to != owner:
                        fault_copy(which, to).start()
                frecv[which] = fsend[:, owner * owned:(owner + 1) * owned, :]

        def last(x, z_term, s4):
            value = us[2][x + 2, PAD:PAD + ny, :]
            return s4 + total(value * (b[x] - half_near(2, x, z_term)))

        wait_y(2)
        s4 = run(last, 2, zero, 1, lambda *p: None)

        slot = lax.broadcasted_iota(jnp.int32, (1, nz), 1)
        sent = jnp.zeros((1, nz), jnp.float32)
        for j, part in enumerate((t0, s0, s1, s2, s3, s4)):
            whole = jnp.sum(jnp.sum(part, axis=1, keepdims=True), axis=0, keepdims=True)
            sent = sent + jnp.where(slot == j, whole, 0.0)
        red[me] = sent

        def sum_copy(step):
            return pltpu.make_async_remote_copy(
                red.at[me], red.at[me], rs_sem.at[step], rr_sem.at[me],
                device_id=other(step), device_id_type=MESH)

        @pl.loop(1, count)
        def _(step):
            sum_copy(step).start()

        @pl.loop(1, count)
        def _(step):
            who = lax.rem(me + step, count)
            pltpu.make_async_remote_copy(
                red.at[who], red.at[who], rs_sem.at[step], rr_sem.at[who],
                device_id=other(step), device_id_type=MESH).wait_recv()

        sums = jnp.sum(red[...], axis=0)
        sums = [jnp.sum(jnp.where(slot == j, sums, 0.0), axis=1, keepdims=True) for j in range(6)]
        coefs = [jnp.broadcast_to(c, (1, nz)) for c in solve(sums[0], sums[1:])]

        def out_copy(c):
            part = pl.ds(c * CHUNK, CHUNK)
            return pltpu.make_async_copy(obuf.at[part], out.at[part], out_sem.at[c])

        def blend(x, carry):
            mid = slice(PAD, PAD + ny)
            obuf[x] = (coefs[0] * u0[x + 2, mid, :] + coefs[1] * u1[x + 2, mid, :]
                       + coefs[2] * u2[x + 2, mid, :])
            return carry

        for c in range(nx // CHUNK):
            lax.fori_loop(c * CHUNK, (c + 1) * CHUNK, blend, 0)
            out_copy(c).start()

        for which, owner in enumerate((ngy // 2 - 1, ngy // 2)):
            @pl.when(iy != owner)
            def _():
                fault_copy(which, owner).wait_recv()
        traction = sum(coefs[j] * (frecv[0, j] + frecv[1, j]) for j in range(3))
        arg = (pre_ref[...] + 2.0 * traction) / norm_ref[...]
        half = jnp.float32(-0.6931471805599453)
        small = arg * (1.0 + arg * arg * (1.0 / 6.0) * (1.0 + arg * arg * 0.05))
        sinh = jnp.where(jnp.abs(arg) < 0.25, small, jnp.exp(arg + half) - jnp.exp(half - arg))
        slip[...] = jnp.exp(-state_ref[...]) * sinh

        for k in range(3):
            each(xcopy, k, ix, ngx, sending, lambda c: c.wait_send())
            each(ycopy, k, iy, ngy, sending, lambda c: c.wait_send())
            for n, (at, size) in enumerate(parts):
                zcopy(k, at, size, n).wait_send()
        for which, owner in enumerate((ngy // 2 - 1, ngy // 2)):
            @pl.when(iy == owner)
            def _():
                for to in range(ngy):
                    if to != owner:
                        fault_copy(which, to).wait_send()

        @pl.loop(1, count)
        def _(step):
            sum_copy(step).wait_send()

        for c in range(nx // CHUNK):
            out_copy(c).wait()

    return kernel


def solution(mesh):
    sizes = tuple(mesh.shape[a] for a in AXES)
    assert sizes[1] % 2 == 0 and sizes[2] == 2

    def per_device(load, stiffness, prestress, state_var, normal_a):
        nx, ny, nz = load.shape
        assert nx % CHUNK == 0
        runs = len(parts_of(nx))
        f32 = jnp.float32
        count = sizes[0] * sizes[1] * sizes[2]
        padded = (nx + 4, ny + 2 * PAD, nz)
        vmem = pl.BlockSpec(memory_space=pltpu.VMEM)
        hbm = pl.BlockSpec(memory_space=pl.ANY)
        dma = pltpu.SemaphoreType.DMA
        return pl.pallas_call(
            make_kernel(sizes),
            out_shape=(
                jax.ShapeDtypeStruct(load.shape, f32),
                jax.ShapeDtypeStruct(prestress.shape, f32),
            ),
            in_specs=[hbm, hbm, vmem, vmem, vmem],
            out_specs=(hbm, vmem),
            scratch_shapes=[
                pltpu.VMEM((nx, ny, nz), f32),
                pltpu.VMEM((nx, ny, nz), f32),
                pltpu.VMEM(padded, f32),
                pltpu.VMEM(padded, f32),
                pltpu.VMEM(padded, f32),
                pltpu.VMEM((nx, ny, nz), f32),
                pltpu.VMEM((3, 2, nx, 2, nz), f32),
                pltpu.VMEM((3, 2, nx, 2, nz), f32),
                pltpu.VMEM((3, nx, ny, nz), f32),
                pltpu.VMEM((2, 4 * nz, nz), jnp.bfloat16),
                pltpu.VMEM((3, nx, nz), f32),
                pltpu.VMEM((2, 3, nx // sizes[1], nz), f32),
                pltpu.VMEM((count, 1, nz), f32),
                dma((2, runs)),
                dma((nx // CHUNK,)),
                dma((3, 4)),
                dma((3, 4)),
                dma((3, runs)),
                dma((3, runs)),
                dma((sizes[1],)),
                dma((2,)),
                dma((count,)),
                dma((count,)),
            ],
            compiler_params=pltpu.CompilerParams(collective_id=0, has_side_effects=True),
        )(load, stiffness, prestress, state_var, normal_a)

    placed = (
        P("gx", "gy", "gz"),
        P("gx", "gy", "gz"),
        P(("gx", "gy"), "gz"),
        P(("gx", "gy"), "gz"),
        P(("gx", "gy"), "gz"),
    )
    return jax.shard_map(
        per_device,
        mesh=mesh,
        in_specs=placed,
        out_specs=(P("gx", "gy", "gz"), P(("gx", "gy"), "gz")),
        check_vma=False,
    )
```

```python
import jax
import jax.numpy as jnp
from jax import lax
from jax.experimental import pallas as pl
from jax.experimental.pallas import tpu as pltpu
from jax.sharding import PartitionSpec as P

MESH = pl.DeviceIdType.MESH
AXES = ("gx", "gy", "gz")
PAD = 8
CHUNK = 8
GROUP = 2


def total(values):
    return jnp.sum(values.reshape(-1, 8, values.shape[-1]), axis=0)


def solve(t0, s):
    t1 = t0 - s[0]
    t2 = t1 - s[1]
    tiny = 1e-7
    p0 = s[0]
    l10 = s[1] / p0
    l20 = s[2] / p0
    p1 = s[2] - l10 * s[1]
    q = s[3] - l20 * s[1]
    ok1 = p1 > tiny * s[2]
    i1 = jnp.where(ok1, 1.0 / jnp.where(ok1, p1, 1.0), 0.0)
    l21 = q * i1
    p2 = s[4] - l20 * s[2] - l21 * q
    ok2 = ok1 & (p2 > tiny * s[4])
    i2 = jnp.where(ok2, 1.0 / jnp.where(ok2, p2, 1.0), 0.0)
    y1 = t1 - l10 * t0
    y2 = t2 - l20 * t0 - l21 * y1
    c2 = y2 * i2
    c1 = y1 * i1 - l21 * c2
    c0 = t0 / p0 - l10 * c1 - l20 * c2
    return c0, c1, c2


def parts_of(nx):
    inner = nx - 4
    runs = max(n for n in range(1, 7) if inner % (GROUP * n) == 0)
    size = inner // runs
    return [(0, 2), (nx - 2, 2)] + [(2 + n * size, size) for n in range(runs)]


def halves(values):
    high = values.astype(jnp.bfloat16)
    return high, (values - high.astype(jnp.float32)).astype(jnp.bfloat16)


def make_kernel(sizes):
    ngx, ngy, ngz = sizes
    count = ngx * ngy * ngz

    def kernel(load, stiff, pre_ref, state_ref, norm_ref, out, slip,
               b, d, u0, u1, u2, obuf, ysend, yrecv, zrecv, band, zterm, fsend, frecv, red,
               in_sem, out_sem, send_sem, recv_sem, zs_sem, zr_sem, fs_sem, fr_sem, rs_sem, rr_sem):
        nx, ny, nz = b.shape
        us = (u0, u1, u2)
        ix, iy, iz = (lax.axis_index(a) for a in AXES)
        me = (ix * ngy + iy) * ngz + iz
        spots = (ix, iy, iz)

        def other(step):
            who = lax.rem(me + step, count)
            return (who // (ngy * ngz), lax.rem(who // ngz, ngy), lax.rem(who, ngz))

        parts = parts_of(nx)
        copies = []
        for n, (at, size) in enumerate(parts):
            part = pl.ds(at, size)
            copies.append((
                pltpu.make_async_copy(load.at[part], b.at[part], in_sem.at[0, n]),
                pltpu.make_async_copy(stiff.at[part], d.at[part], in_sem.at[1, n]),
            ))
            for one in copies[n]:
                one.start()

        barrier = pltpu.get_barrier_semaphore()

        @pl.loop(1, count)
        def _(step):
            pl.semaphore_signal(barrier, inc=1, device_id=other(step), device_id_type=MESH)

        zero_plane = jnp.zeros((2, ny, nz), jnp.float32)
        zero_rows = jnp.zeros((nx, 2, nz), jnp.float32)
        for k in range(3):
            @pl.when(ix == 0)
            def _():
                us[k][0:2, PAD:PAD + ny, :] = zero_plane
            @pl.when(ix == ngx - 1)
            def _():
                us[k][nx + 2:nx + 4, PAD:PAD + ny, :] = zero_plane
            @pl.when(iy == 0)
            def _():
                yrecv[k, 0] = zero_rows
            @pl.when(iy == ngy - 1)
            def _():
                yrecv[k, 1] = zero_rows

        row = lax.broadcasted_iota(jnp.int32, (nz, nz), 0)
        col = lax.broadcasted_iota(jnp.int32, (nz, nz), 1)
        far = row + jnp.where(iz == 0, nz, -nz)
        for n, at in enumerate((row, far, row, far)):
            gap = col - at
            full = jnp.where(jnp.abs(gap) == 1, 16.0, 0.0) - jnp.where(jnp.abs(gap) == 2, 1.0, 0.0)
            half = jnp.where(gap == 1, 16.0, 0.0) - jnp.where(gap == 2, 1.0, 0.0)
            band[0, n * nz:(n + 1) * nz, :] = full.astype(jnp.bfloat16)
            band[1, n * nz:(n + 1) * nz, :] = half.astype(jnp.bfloat16)

        def place(x, value, k):
            us[k][x + 2, PAD:PAD + ny, :] = value
            ysend[k, 0, x] = value[0:2]
            ysend[k, 1, x] = value[ny - 2:ny]

        def xcopy(k, side):
            u = us[k]
            if side == 0:
                src, dst, to = u.at[2:4, PAD:PAD + ny], u.at[nx + 2:nx + 4, PAD:PAD + ny], ix - 1
            else:
                src, dst, to = u.at[nx:nx + 2, PAD:PAD + ny], u.at[0:2, PAD:PAD + ny], ix + 1
            return pltpu.make_async_remote_copy(
                src, dst, send_sem.at[k, side], recv_sem.at[k, side],
                device_id=(to, iy, iz), device_id_type=MESH)

        def ycopy(k, side):
            to = iy - 1 if side == 0 else iy + 1
            return pltpu.make_async_remote_copy(
                ysend.at[k, side], yrecv.at[k, 1 - side], send_sem.at[k, 2 + side],
                recv_sem.at[k, 2 + side], device_id=(ix, to, iz), device_id_type=MESH)

        strips = ((8, ny - 8), (0, 8), (ny - 8, ny))

        def zcopy(k, at, size, n, strip):
            lo, hi = (0, ny) if strip is None else strips[strip]
            which = 0 if strip is None else strip
            return pltpu.make_async_remote_copy(
                us[k].at[pl.ds(at + 2, size), PAD + lo:PAD + hi], zrecv.at[k, pl.ds(at, size), lo:hi],
                zs_sem.at[k, n, which], zr_sem.at[k, n, which],
                device_id=(ix, iy, 1 - iz), device_id_type=MESH)

        def strips_of(n):
            return (None,) if n < 2 else (0, 1, 2)

        def sending(spot, size, side):
            return spot > 0 if side == 0 else spot < size - 1

        def receiving(spot, size, side):
            return spot < size - 1 if side == 0 else spot > 0

        def sides(k):
            return (1,) if k == 2 else (0, 1)

        def each(make, k, spot, size, test, act):
            for side in sides(k):
                @pl.when(test(spot, size, side))
                def _():
                    act(make(k, side))

        def start_x(k):
            each(xcopy, k, ix, ngx, sending, lambda c: c.start())

        def start_y(k):
            each(ycopy, k, iy, ngy, sending, lambda c: c.start())

        def scale(x, t0):
            inv = 1.0 / (7.5 + d[x])
            d[x] = inv
            rhs = b[x]
            value = inv * rhs
            place(x, value, 0)
            return t0 + total(value * rhs)

        t0 = jnp.zeros((8, nz), jnp.float32)
        for n, (at, size) in enumerate(parts):
            for one in copies[n]:
                one.wait()
            t0 = lax.fori_loop(at, at + size, scale, t0)
            if n == 1:
                pl.semaphore_wait(barrier, count - 1)
                start_x(0)
                zcopy(0, *parts[0], 0, None).start()
            if n >= 1:
                for strip in strips_of(n):
                    zcopy(0, at, size, n, strip).start()
        start_y(0)

        def wait_y(k):
            each(ycopy, k, iy, ngy, receiving, lambda c: c.wait_recv())

        def wait_x(k):
            each(xcopy, k, ix, ngx, receiving, lambda c: c.wait_recv())

        def along_z(k, at, size, lo, hi, which):
            rows = size * (hi - lo)
            own = us[k][pl.ds(at + 2, size), PAD + lo:PAD + hi, :].reshape(rows, nz)
            next_to = zrecv[k, pl.ds(at, size), lo:hi, :].reshape(rows, nz)
            own_high, own_low = halves(own)
            next_high, next_low = halves(next_to)
            lhs = jnp.concatenate([own_high, next_high, own_low, next_low], axis=1)
            found = jnp.dot(lhs, band[which], preferred_element_type=jnp.float32)
            zterm[pl.ds(at, size), lo:hi, :] = found.reshape(size, hi - lo, nz)

        def near(k, x, lo, hi):
            u = us[k]
            lo, hi = lo + PAD, hi + PAD
            one = (u[x + 1, lo:hi, :] + u[x + 3, lo:hi, :]
                   + u[x + 2, lo - 1:hi - 1, :] + u[x + 2, lo + 1:hi + 1, :])
            two = (u[x, lo:hi, :] + u[x + 4, lo:hi, :]
                   + u[x + 2, lo - 2:hi - 2, :] + u[x + 2, lo + 2:hi + 2, :])
            return (16.0 * one - two + zterm[x, lo - PAD:hi - PAD, :]) * (1.0 / 12.0)

        def half_near(k, x, lo, hi):
            u = us[k]
            lo, hi = lo + PAD, hi + PAD
            one = u[x + 1, lo:hi, :] + u[x + 2, lo - 1:hi - 1, :]
            two = u[x, lo:hi, :] + u[x + 2, lo - 2:hi - 2, :]
            return (16.0 * one - two + zterm[x, lo - PAD:hi - PAD, :]) * (1.0 / 6.0)

        zero = jnp.zeros((8, nz), jnp.float32)

        def run(block, k, carry, which, finish):
            first_at, size = parts[2]

            def part(n, carry):
                at = first_at + n * size
                zcopy(k, at, size, n + 2, 0).wait_recv()
                along_z(k, at, size, *strips[0], which)

                def inner(i, carry):
                    for g in range(GROUP):
                        carry = block(at + i * GROUP + g, *strips[0], carry)
                    return carry

                carry = lax.fori_loop(0, size // GROUP, inner, carry)
                if k < 2:
                    zcopy(k + 1, at, size, n + 2, 0).start()
                return carry

            carry = lax.fori_loop(0, len(parts) - 2, part, carry)
            for n, (at, size) in enumerate(parts):
                for strip in strips_of(n):
                    if strip != 0:
                        zcopy(k, at, size, n, strip).wait_recv()
                if n < 2:
                    along_z(k, at, size, 0, ny, which)
            for strip in (1, 2):
                along_z(k, 2, nx - 4, *strips[strip], which)
            wait_y(k)

            def rim(i, carry):
                for g in range(GROUP):
                    x = i * GROUP + g
                    us[k][x + 2, PAD - 2:PAD, :] = yrecv[k, 0, x]
                    us[k][x + 2, PAD + ny:PAD + ny + 2, :] = yrecv[k, 1, x]
                    carry = block(x, 0, 8, carry)
                    carry = block(x, ny - 8, ny, carry)
                return carry

            def whole(n, carry):
                x = jnp.where(n < 2, n, nx - 4 + n)
                us[k][x + 2, PAD - 2:PAD, :] = yrecv[k, 0, x]
                us[k][x + 2, PAD + ny:PAD + ny + 2, :] = yrecv[k, 1, x]
                carry = block(x, 0, ny, carry)
                return carry

            carry = lax.fori_loop(1, nx // GROUP - 1, rim, carry)
            wait_x(k)
            carry = lax.fori_loop(0, 4, whole, carry)
            finish()
            return carry

        def advance(k):
            def block(x, lo, hi, carry):
                even, odd = carry
                value = us[k][x + 2, PAD + lo:PAD + hi, :]
                w = near(k, x, lo, hi)
                fresh = d[x, lo:hi, :] * w
                even = even + total(value * (b[x, lo:hi, :] - w))
                odd = odd + total((value - fresh) * w)
                b[x, lo:hi, :] = w
                us[k + 1][x + 2, PAD + lo:PAD + hi, :] = fresh
                if lo == 0:
                    ysend[k + 1, 0, x] = fresh[0:2]
                if hi == ny:
                    ysend[k + 1, 1, x] = fresh[hi - lo - 2:hi - lo]
                return even, odd

            def finish():
                start_x(k + 1)
                start_y(k + 1)
                for n, (at, size) in enumerate(parts):
                    for strip in strips_of(n):
                        if strip != 0:
                            zcopy(k + 1, at, size, n, strip).start()

            return run(block, k, (zero, zero), 0, finish)

        s0, s1 = advance(0)
        s2, s3 = advance(1)

        owned = nx // ngy
        below = iy == ngy // 2 - 1
        above = iy == ngy // 2

        def fault_copy(which, to):
            return pltpu.make_async_remote_copy(
                fsend.at[:, pl.ds(to * owned, owned), :], frecv.at[which], fs_sem.at[to], fr_sem.at[which],
                device_id=(ix, to, iz), device_id_type=MESH)

        @pl.when(below | above)
        def _():
            edge = jnp.where(below, 1, 0)
            front = jnp.where(below, 1.0 / 24.0, 27.0 / 24.0)
            close = jnp.where(below, -27.0 / 24.0, -1.0 / 24.0)

            @pl.loop(0, nx)
            def _(x):
                for j in range(3):
                    rows = ysend[j, edge, x]
                    fsend[j, pl.ds(x, 1), :] = front * rows[0:1] + close * rows[1:2]

        for which, owner in enumerate((ngy // 2 - 1, ngy // 2)):
            @pl.when(iy == owner)
            def _():
                for to in range(ngy):
                    if to != owner:
                        fault_copy(which, to).start()
                frecv[which] = fsend[:, owner * owned:(owner + 1) * owned, :]

        def last(x, lo, hi, s4):
            value = us[2][x + 2, PAD + lo:PAD + hi, :]
            return s4 + total(value * (b[x, lo:hi, :] - half_near(2, x, lo, hi)))

        s4 = run(last, 2, zero, 1, lambda: None)

        slot = lax.broadcasted_iota(jnp.int32, (1, nz), 1)
        sent = jnp.zeros((1, nz), jnp.float32)
        for j, part in enumerate((t0, s0, s1, s2, s3, s4)):
            whole = jnp.sum(jnp.sum(part, axis=1, keepdims=True), axis=0, keepdims=True)
            sent = sent + jnp.where(slot == j, whole, 0.0)
        red[me] = sent

        def sum_copy(step):
            return pltpu.make_async_remote_copy(
                red.at[me], red.at[me], rs_sem.at[step], rr_sem.at[me],
                device_id=other(step), device_id_type=MESH)

        @pl.loop(1, count)
        def _(step):
            sum_copy(step).start()

        @pl.loop(1, count)
        def _(step):
            who = lax.rem(me + step, count)
            pltpu.make_async_remote_copy(
                red.at[who], red.at[who], rs_sem.at[step], rr_sem.at[who],
                device_id=other(step), device_id_type=MESH).wait_recv()

        sums = jnp.sum(red[...], axis=0)
        sums = [jnp.sum(jnp.where(slot == j, sums, 0.0), axis=1, keepdims=True) for j in range(6)]
        coefs = [jnp.broadcast_to(c, (1, nz)) for c in solve(sums[0], sums[1:])]

        def out_copy(c):
            part = pl.ds(c * CHUNK, CHUNK)
            return pltpu.make_async_copy(obuf.at[part], out.at[part], out_sem.at[c])

        def blend(x, carry):
            mid = slice(PAD, PAD + ny)
            obuf[x] = (coefs[0] * u0[x + 2, mid, :] + coefs[1] * u1[x + 2, mid, :]
                       + coefs[2] * u2[x + 2, mid, :])
            return carry

        for c in range(nx // CHUNK):
            lax.fori_loop(c * CHUNK, (c + 1) * CHUNK, blend, 0)
            out_copy(c).start()

        for which, owner in enumerate((ngy // 2 - 1, ngy // 2)):
            @pl.when(iy != owner)
            def _():
                fault_copy(which, owner).wait_recv()
        traction = sum(coefs[j] * (frecv[0, j] + frecv[1, j]) for j in range(3))
        arg = (pre_ref[...] + 2.0 * traction) / norm_ref[...]
        half = jnp.float32(-0.6931471805599453)
        small = arg * (1.0 + arg * arg * (1.0 / 6.0) * (1.0 + arg * arg * 0.05))
        sinh = jnp.where(jnp.abs(arg) < 0.25, small, jnp.exp(arg + half) - jnp.exp(half - arg))
        slip[...] = jnp.exp(-state_ref[...]) * sinh

        for k in range(3):
            each(xcopy, k, ix, ngx, sending, lambda c: c.wait_send())
            each(ycopy, k, iy, ngy, sending, lambda c: c.wait_send())
            for n, (at, size) in enumerate(parts):
                for strip in strips_of(n):
                    zcopy(k, at, size, n, strip).wait_send()
        for which, owner in enumerate((ngy // 2 - 1, ngy // 2)):
            @pl.when(iy == owner)
            def _():
                for to in range(ngy):
                    if to != owner:
                        fault_copy(which, to).wait_send()

        @pl.loop(1, count)
        def _(step):
            sum_copy(step).wait_send()

        for c in range(nx // CHUNK):
            out_copy(c).wait()

    return kernel


def solution(mesh):
    sizes = tuple(mesh.shape[a] for a in AXES)
    assert sizes[1] % 2 == 0 and sizes[2] == 2

    def per_device(load, stiffness, prestress, state_var, normal_a):
        nx, ny, nz = load.shape
        assert nx % CHUNK == 0
        runs = len(parts_of(nx))
        f32 = jnp.float32
        count = sizes[0] * sizes[1] * sizes[2]
        padded = (nx + 4, ny + 2 * PAD, nz)
        vmem = pl.BlockSpec(memory_space=pltpu.VMEM)
        hbm = pl.BlockSpec(memory_space=pl.ANY)
        dma = pltpu.SemaphoreType.DMA
        return pl.pallas_call(
            make_kernel(sizes),
            out_shape=(
                jax.ShapeDtypeStruct(load.shape, f32),
                jax.ShapeDtypeStruct(prestress.shape, f32),
            ),
            in_specs=[hbm, hbm, vmem, vmem, vmem],
            out_specs=(hbm, vmem),
            scratch_shapes=[
                pltpu.VMEM((nx, ny, nz), f32),
                pltpu.VMEM((nx, ny, nz), f32),
                pltpu.VMEM(padded, f32),
                pltpu.VMEM(padded, f32),
                pltpu.VMEM(padded, f32),
                pltpu.VMEM((nx, ny, nz), f32),
                pltpu.VMEM((3, 2, nx, 2, nz), f32),
                pltpu.VMEM((3, 2, nx, 2, nz), f32),
                pltpu.VMEM((3, nx, ny, nz), f32),
                pltpu.VMEM((2, 4 * nz, nz), jnp.bfloat16),
                pltpu.VMEM((nx, ny, nz), f32),
                pltpu.VMEM((3, nx, nz), f32),
                pltpu.VMEM((2, 3, nx // sizes[1], nz), f32),
                pltpu.VMEM((count, 1, nz), f32),
                dma((2, runs)),
                dma((nx // CHUNK,)),
                dma((3, 4)),
                dma((3, 4)),
                dma((3, runs, 3)),
                dma((3, runs, 3)),
                dma((sizes[1],)),
                dma((2,)),
                dma((count,)),
                dma((count,)),
            ],
            compiler_params=pltpu.CompilerParams(collective_id=0, has_side_effects=True),
        )(load, stiffness, prestress, state_var, normal_a)

    placed = (
        P("gx", "gy", "gz"),
        P("gx", "gy", "gz"),
        P(("gx", "gy"), "gz"),
        P(("gx", "gy"), "gz"),
        P(("gx", "gy"), "gz"),
    )
    return jax.shard_map(
        per_device,
        mesh=mesh,
        in_specs=placed,
        out_specs=(P("gx", "gy", "gz"), P(("gx", "gy"), "gz")),
        check_vma=False,
    )
```

```python
import jax
import jax.numpy as jnp
from jax import lax
from jax.experimental import pallas as pl
from jax.experimental.pallas import tpu as pltpu
from jax.sharding import PartitionSpec as P

MESH = pl.DeviceIdType.MESH
AXES = ("gx", "gy", "gz")
PAD = 8
CHUNK = 8
GROUP = 2


def total(values):
    return jnp.sum(values.reshape(-1, 8, values.shape[-1]), axis=0)


def solve(t0, s):
    t1 = t0 - s[0]
    t2 = t1 - s[1]
    tiny = 1e-7
    p0 = s[0]
    l10 = s[1] / p0
    l20 = s[2] / p0
    p1 = s[2] - l10 * s[1]
    q = s[3] - l20 * s[1]
    ok1 = p1 > tiny * s[2]
    i1 = jnp.where(ok1, 1.0 / jnp.where(ok1, p1, 1.0), 0.0)
    l21 = q * i1
    p2 = s[4] - l20 * s[2] - l21 * q
    ok2 = ok1 & (p2 > tiny * s[4])
    i2 = jnp.where(ok2, 1.0 / jnp.where(ok2, p2, 1.0), 0.0)
    y1 = t1 - l10 * t0
    y2 = t2 - l20 * t0 - l21 * y1
    c2 = y2 * i2
    c1 = y1 * i1 - l21 * c2
    c0 = t0 / p0 - l10 * c1 - l20 * c2
    return c0, c1, c2


def parts_of(nx):
    inner = nx - 4
    runs = max(n for n in range(1, 7) if inner % (GROUP * n) == 0)
    size = inner // runs
    return [(0, 2), (nx - 2, 2)] + [(2 + n * size, size) for n in range(runs)]


def halves(values):
    high = values.astype(jnp.bfloat16)
    return high, (values - high.astype(jnp.float32)).astype(jnp.bfloat16)


def make_kernel(sizes):
    ngx, ngy, ngz = sizes
    count = ngx * ngy * ngz

    def kernel(load, stiff, pre_ref, state_ref, norm_ref, u0, u1, u2, coef_ref, slip,
               b, d, ysend, yrecv, zrecv, band, zterm, fsend, frecv, red,
               in_sem, send_sem, recv_sem, zs_sem, zr_sem, fs_sem, fr_sem, rs_sem, rr_sem):
        nx, ny, nz = b.shape
        us = (u0, u1, u2)
        ix, iy, iz = (lax.axis_index(a) for a in AXES)
        me = (ix * ngy + iy) * ngz + iz
        spots = (ix, iy, iz)

        def other(step):
            who = lax.rem(me + step, count)
            return (who // (ngy * ngz), lax.rem(who // ngz, ngy), lax.rem(who, ngz))

        parts = parts_of(nx)
        copies = []
        for n, (at, size) in enumerate(parts):
            part = pl.ds(at, size)
            copies.append((
                pltpu.make_async_copy(load.at[part], b.at[part], in_sem.at[0, n]),
                pltpu.make_async_copy(stiff.at[part], d.at[part], in_sem.at[1, n]),
            ))
            for one in copies[n]:
                one.start()

        barrier = pltpu.get_barrier_semaphore()

        @pl.loop(1, count)
        def _(step):
            pl.semaphore_signal(barrier, inc=1, device_id=other(step), device_id_type=MESH)

        zero_plane = jnp.zeros((2, ny, nz), jnp.float32)
        zero_rows = jnp.zeros((nx, 2, nz), jnp.float32)
        for k in range(3):
            @pl.when(ix == 0)
            def _():
                us[k][0:2, PAD:PAD + ny, :] = zero_plane
            @pl.when(ix == ngx - 1)
            def _():
                us[k][nx + 2:nx + 4, PAD:PAD + ny, :] = zero_plane
            @pl.when(iy == 0)
            def _():
                yrecv[k, 0] = zero_rows
            @pl.when(iy == ngy - 1)
            def _():
                yrecv[k, 1] = zero_rows

        row = lax.broadcasted_iota(jnp.int32, (nz, nz), 0)
        col = lax.broadcasted_iota(jnp.int32, (nz, nz), 1)
        far = row + jnp.where(iz == 0, nz, -nz)
        for n, at in enumerate((row, far, row, far)):
            gap = col - at
            full = jnp.where(jnp.abs(gap) == 1, 16.0, 0.0) - jnp.where(jnp.abs(gap) == 2, 1.0, 0.0)
            half = jnp.where(gap == 1, 16.0, 0.0) - jnp.where(gap == 2, 1.0, 0.0)
            band[0, n * nz:(n + 1) * nz, :] = full.astype(jnp.bfloat16)
            band[1, n * nz:(n + 1) * nz, :] = half.astype(jnp.bfloat16)

        def place(x, value, k):
            us[k][x + 2, PAD:PAD + ny, :] = value
            ysend[k, 0, x] = value[0:2]
            ysend[k, 1, x] = value[ny - 2:ny]

        def xcopy(k, side):
            u = us[k]
            if side == 0:
                src, dst, to = u.at[2:4, PAD:PAD + ny], u.at[nx + 2:nx + 4, PAD:PAD + ny], ix - 1
            else:
                src, dst, to = u.at[nx:nx + 2, PAD:PAD + ny], u.at[0:2, PAD:PAD + ny], ix + 1
            return pltpu.make_async_remote_copy(
                src, dst, send_sem.at[k, side], recv_sem.at[k, side],
                device_id=(to, iy, iz), device_id_type=MESH)

        def ycopy(k, side):
            to = iy - 1 if side == 0 else iy + 1
            return pltpu.make_async_remote_copy(
                ysend.at[k, side], yrecv.at[k, 1 - side], send_sem.at[k, 2 + side],
                recv_sem.at[k, 2 + side], device_id=(ix, to, iz), device_id_type=MESH)

        strips = ((8, ny - 8), (0, 8), (ny - 8, ny))

        def zcopy(k, at, size, n, strip):
            lo, hi = (0, ny) if strip is None else strips[strip]
            which = 0 if strip is None else strip
            return pltpu.make_async_remote_copy(
                us[k].at[pl.ds(at + 2, size), PAD + lo:PAD + hi], zrecv.at[k, pl.ds(at, size), lo:hi],
                zs_sem.at[k, n, which], zr_sem.at[k, n, which],
                device_id=(ix, iy, 1 - iz), device_id_type=MESH)

        def strips_of(n):
            return (None,) if n < 2 else (0, 1, 2)

        def sending(spot, size, side):
            return spot > 0 if side == 0 else spot < size - 1

        def receiving(spot, size, side):
            return spot < size - 1 if side == 0 else spot > 0

        def sides(k):
            return (1,) if k == 2 else (0, 1)

        def each(make, k, spot, size, test, act):
            for side in sides(k):
                @pl.when(test(spot, size, side))
                def _():
                    act(make(k, side))

        def start_x(k):
            each(xcopy, k, ix, ngx, sending, lambda c: c.start())

        def start_y(k):
            each(ycopy, k, iy, ngy, sending, lambda c: c.start())

        def scale(x, t0):
            inv = 1.0 / (7.5 + d[x])
            d[x] = inv
            rhs = b[x]
            value = inv * rhs
            place(x, value, 0)
            return t0 + total(value * rhs)

        t0 = jnp.zeros((8, nz), jnp.float32)
        for n, (at, size) in enumerate(parts):
            for one in copies[n]:
                one.wait()
            t0 = lax.fori_loop(at, at + size, scale, t0)
            if n == 1:
                pl.semaphore_wait(barrier, count - 1)
                start_x(0)
                zcopy(0, *parts[0], 0, None).start()
            if n >= 1:
                for strip in strips_of(n):
                    zcopy(0, at, size, n, strip).start()
        start_y(0)

        def wait_y(k):
            each(ycopy, k, iy, ngy, receiving, lambda c: c.wait_recv())

        def wait_x(k):
            each(xcopy, k, ix, ngx, receiving, lambda c: c.wait_recv())

        def along_z(k, at, size, lo, hi, which):
            rows = size * (hi - lo)
            own = us[k][pl.ds(at + 2, size), PAD + lo:PAD + hi, :].reshape(rows, nz)
            next_to = zrecv[k, pl.ds(at, size), lo:hi, :].reshape(rows, nz)
            own_high, own_low = halves(own)
            next_high, next_low = halves(next_to)
            lhs = jnp.concatenate([own_high, next_high, own_low, next_low], axis=1)
            found = jnp.dot(lhs, band[which], preferred_element_type=jnp.float32)
            zterm[pl.ds(at, size), lo:hi, :] = found.reshape(size, hi - lo, nz)

        def near(k, x, lo, hi):
            u = us[k]
            lo, hi = lo + PAD, hi + PAD
            one = (u[x + 1, lo:hi, :] + u[x + 3, lo:hi, :]
                   + u[x + 2, lo - 1:hi - 1, :] + u[x + 2, lo + 1:hi + 1, :])
            two = (u[x, lo:hi, :] + u[x + 4, lo:hi, :]
                   + u[x + 2, lo - 2:hi - 2, :] + u[x + 2, lo + 2:hi + 2, :])
            return (16.0 * one - two + zterm[x, lo - PAD:hi - PAD, :]) * (1.0 / 12.0)

        def half_near(k, x, lo, hi):
            u = us[k]
            lo, hi = lo + PAD, hi + PAD
            one = u[x + 1, lo:hi, :] + u[x + 2, lo - 1:hi - 1, :]
            two = u[x, lo:hi, :] + u[x + 2, lo - 2:hi - 2, :]
            return (16.0 * one - two + zterm[x, lo - PAD:hi - PAD, :]) * (1.0 / 6.0)

        zero = jnp.zeros((8, nz), jnp.float32)

        def run(block, k, carry, which, finish):
            first_at, size = parts[2]

            def part(n, carry):
                at = first_at + n * size
                zcopy(k, at, size, n + 2, 0).wait_recv()
                along_z(k, at, size, *strips[0], which)

                def inner(i, carry):
                    for g in range(GROUP):
                        carry = block(at + i * GROUP + g, *strips[0], carry)
                    return carry

                carry = lax.fori_loop(0, size // GROUP, inner, carry)
                if k < 2:
                    zcopy(k + 1, at, size, n + 2, 0).start()
                return carry

            carry = lax.fori_loop(0, len(parts) - 2, part, carry)
            for n, (at, size) in enumerate(parts):
                for strip in strips_of(n):
                    if strip != 0:
                        zcopy(k, at, size, n, strip).wait_recv()
                if n < 2:
                    along_z(k, at, size, 0, ny, which)
            for strip in (1, 2):
                along_z(k, 2, nx - 4, *strips[strip], which)
            wait_y(k)

            def rim(i, carry):
                for g in range(GROUP):
                    x = i * GROUP + g
                    us[k][x + 2, PAD - 2:PAD, :] = yrecv[k, 0, x]
                    us[k][x + 2, PAD + ny:PAD + ny + 2, :] = yrecv[k, 1, x]
                    carry = block(x, 0, 8, carry)
                    carry = block(x, ny - 8, ny, carry)
                return carry

            def whole(n, carry):
                x = jnp.where(n < 2, n, nx - 4 + n)
                us[k][x + 2, PAD - 2:PAD, :] = yrecv[k, 0, x]
                us[k][x + 2, PAD + ny:PAD + ny + 2, :] = yrecv[k, 1, x]
                carry = block(x, 0, ny, carry)
                return carry

            carry = lax.fori_loop(1, nx // GROUP - 1, rim, carry)
            wait_x(k)
            carry = lax.fori_loop(0, 4, whole, carry)
            finish()
            return carry

        def advance(k):
            def block(x, lo, hi, carry):
                even, odd = carry
                value = us[k][x + 2, PAD + lo:PAD + hi, :]
                w = near(k, x, lo, hi)
                fresh = d[x, lo:hi, :] * w
                even = even + total(value * (b[x, lo:hi, :] - w))
                odd = odd + total((value - fresh) * w)
                b[x, lo:hi, :] = w
                us[k + 1][x + 2, PAD + lo:PAD + hi, :] = fresh
                if lo == 0:
                    ysend[k + 1, 0, x] = fresh[0:2]
                if hi == ny:
                    ysend[k + 1, 1, x] = fresh[hi - lo - 2:hi - lo]
                return even, odd

            def finish():
                start_x(k + 1)
                start_y(k + 1)
                for n, (at, size) in enumerate(parts):
                    for strip in strips_of(n):
                        if strip != 0:
                            zcopy(k + 1, at, size, n, strip).start()

            return run(block, k, (zero, zero), 0, finish)

        s0, s1 = advance(0)
        s2, s3 = advance(1)

        owned = nx // ngy
        below = iy == ngy // 2 - 1
        above = iy == ngy // 2

        def fault_copy(which, to):
            return pltpu.make_async_remote_copy(
                fsend.at[:, pl.ds(to * owned, owned), :], frecv.at[which], fs_sem.at[to], fr_sem.at[which],
                device_id=(ix, to, iz), device_id_type=MESH)

        @pl.when(below | above)
        def _():
            edge = jnp.where(below, 1, 0)
            front = jnp.where(below, 1.0 / 24.0, 27.0 / 24.0)
            close = jnp.where(below, -27.0 / 24.0, -1.0 / 24.0)

            @pl.loop(0, nx)
            def _(x):
                for j in range(3):
                    rows = ysend[j, edge, x]
                    fsend[j, pl.ds(x, 1), :] = front * rows[0:1] + close * rows[1:2]

        for which, owner in enumerate((ngy // 2 - 1, ngy // 2)):
            @pl.when(iy == owner)
            def _():
                for to in range(ngy):
                    if to != owner:
                        fault_copy(which, to).start()
                frecv[which] = fsend[:, owner * owned:(owner + 1) * owned, :]

        def last(x, lo, hi, s4):
            value = us[2][x + 2, PAD + lo:PAD + hi, :]
            return s4 + total(value * (b[x, lo:hi, :] - half_near(2, x, lo, hi)))

        s4 = run(last, 2, zero, 1, lambda: None)

        slot = lax.broadcasted_iota(jnp.int32, (1, nz), 1)
        sent = jnp.zeros((1, nz), jnp.float32)
        for j, part in enumerate((t0, s0, s1, s2, s3, s4)):
            whole = jnp.sum(jnp.sum(part, axis=1, keepdims=True), axis=0, keepdims=True)
            sent = sent + jnp.where(slot == j, whole, 0.0)
        red[me] = sent

        def sum_copy(step):
            return pltpu.make_async_remote_copy(
                red.at[me], red.at[me], rs_sem.at[step], rr_sem.at[me],
                device_id=other(step), device_id_type=MESH)

        @pl.loop(1, count)
        def _(step):
            sum_copy(step).start()

        @pl.loop(1, count)
        def _(step):
            who = lax.rem(me + step, count)
            pltpu.make_async_remote_copy(
                red.at[who], red.at[who], rs_sem.at[step], rr_sem.at[who],
                device_id=other(step), device_id_type=MESH).wait_recv()

        sums = jnp.sum(red[...], axis=0)
        sums = [jnp.sum(jnp.where(slot == j, sums, 0.0), axis=1, keepdims=True) for j in range(6)]
        coefs = [jnp.broadcast_to(c, (1, nz)) for c in solve(sums[0], sums[1:])]

        for j in range(3):
            coef_ref[j:j + 1, :] = coefs[j]

        for which, owner in enumerate((ngy // 2 - 1, ngy // 2)):
            @pl.when(iy != owner)
            def _():
                fault_copy(which, owner).wait_recv()
        traction = sum(coefs[j] * (frecv[0, j] + frecv[1, j]) for j in range(3))
        arg = (pre_ref[...] + 2.0 * traction) / norm_ref[...]
        half = jnp.float32(-0.6931471805599453)
        small = arg * (1.0 + arg * arg * (1.0 / 6.0) * (1.0 + arg * arg * 0.05))
        sinh = jnp.where(jnp.abs(arg) < 0.25, small, jnp.exp(arg + half) - jnp.exp(half - arg))
        slip[...] = jnp.exp(-state_ref[...]) * sinh

        for k in range(3):
            each(xcopy, k, ix, ngx, sending, lambda c: c.wait_send())
            each(ycopy, k, iy, ngy, sending, lambda c: c.wait_send())
            for n, (at, size) in enumerate(parts):
                for strip in strips_of(n):
                    zcopy(k, at, size, n, strip).wait_send()
        for which, owner in enumerate((ngy // 2 - 1, ngy // 2)):
            @pl.when(iy == owner)
            def _():
                for to in range(ngy):
                    if to != owner:
                        fault_copy(which, to).wait_send()

        @pl.loop(1, count)
        def _(step):
            sum_copy(step).wait_send()

    return kernel


def blend(u0, u1, u2, coef_ref, out, obuf, out_sem):
    nx, ny, nz = obuf.shape
    mid = slice(PAD, PAD + ny)
    coefs = [coef_ref[j:j + 1, :] for j in range(3)]

    def out_copy(c):
        part = pl.ds(c * CHUNK, CHUNK)
        return pltpu.make_async_copy(obuf.at[part], out.at[part], out_sem.at[c])

    def plane(x, carry):
        obuf[x] = (coefs[0] * u0[x + 2, mid, :] + coefs[1] * u1[x + 2, mid, :]
                   + coefs[2] * u2[x + 2, mid, :])
        return carry

    for c in range(nx // CHUNK):
        lax.fori_loop(c * CHUNK, (c + 1) * CHUNK, plane, 0)
        out_copy(c).start()
    for c in range(nx // CHUNK):
        out_copy(c).wait()


def solution(mesh):
    sizes = tuple(mesh.shape[a] for a in AXES)
    assert sizes[1] % 2 == 0 and sizes[2] == 2

    def per_device(load, stiffness, prestress, state_var, normal_a):
        nx, ny, nz = load.shape
        assert nx % CHUNK == 0
        runs = len(parts_of(nx))
        f32 = jnp.float32
        count = sizes[0] * sizes[1] * sizes[2]
        padded = (nx + 4, ny + 2 * PAD, nz)
        vmem = pl.BlockSpec(memory_space=pltpu.VMEM)
        hbm = pl.BlockSpec(memory_space=pltpu.HBM)
        dma = pltpu.SemaphoreType.DMA
        u0, u1, u2, coefs, slip = pl.pallas_call(
            make_kernel(sizes),
            out_shape=(
                pltpu.VMEM(padded, f32),
                pltpu.VMEM(padded, f32),
                pltpu.VMEM(padded, f32),
                pltpu.VMEM((8, nz), f32),
                jax.ShapeDtypeStruct(prestress.shape, f32),
            ),
            in_specs=[hbm, hbm, vmem, vmem, vmem],
            out_specs=(vmem,) * 5,
            scratch_shapes=[
                pltpu.VMEM((nx, ny, nz), f32),
                pltpu.VMEM((nx, ny, nz), f32),
                pltpu.VMEM((3, 2, nx, 2, nz), f32),
                pltpu.VMEM((3, 2, nx, 2, nz), f32),
                pltpu.VMEM((3, nx, ny, nz), f32),
                pltpu.VMEM((2, 4 * nz, nz), jnp.bfloat16),
                pltpu.VMEM((nx, ny, nz), f32),
                pltpu.VMEM((3, nx, nz), f32),
                pltpu.VMEM((2, 3, nx // sizes[1], nz), f32),
                pltpu.VMEM((count, 1, nz), f32),
                dma((2, runs)),
                dma((3, 4)),
                dma((3, 4)),
                dma((3, runs, 3)),
                dma((3, runs, 3)),
                dma((sizes[1],)),
                dma((2,)),
                dma((count,)),
                dma((count,)),
            ],
            compiler_params=pltpu.CompilerParams(
                collective_id=0, has_side_effects=True, vmem_limit_bytes=54 * 2**20),
        )(load, stiffness, prestress, state_var, normal_a)
        displacement = pl.pallas_call(
            blend,
            out_shape=jax.ShapeDtypeStruct(load.shape, f32),
            in_specs=[vmem] * 4,
            out_specs=hbm,
            scratch_shapes=[pltpu.VMEM((nx, ny, nz), f32), dma((nx // CHUNK,))],
            compiler_params=pltpu.CompilerParams(vmem_limit_bytes=8 * 2**20),
        )(u0, u1, u2, coefs)
        return displacement, slip

    placed = (
        P("gx", "gy", "gz"),
        P("gx", "gy", "gz"),
        P(("gx", "gy"), "gz"),
        P(("gx", "gy"), "gz"),
        P(("gx", "gy"), "gz"),
    )
    return jax.shard_map(
        per_device,
        mesh=mesh,
        in_specs=placed,
        out_specs=(P("gx", "gy", "gz"), P(("gx", "gy"), "gz")),
        check_vma=False,
    )
```
